32 devices in a mesh: cells: 8 (over y, x, core), wells: 4 (over z).
Axes of the slice: x: 2, y: 2, z: 4, core: 2. Of those that a mesh axis runs over, the one named last changes fastest.
Arguments:
- cell_state: float32 [3, 4, 131072], P(None, 'wells', 'cells'), may hold values from -6 to 6
- cell_residual: float32 [3, 4, 131072], P(None, 'wells', 'cells'), may hold values from -6 to 6
- cell_block: float32 [9, 4, 131072], P(None, 'wells', 'cells'), may hold values from -4 to 4
- block_inverse: float32 [9, 4, 131072], P(None, 'wells', 'cells'), may hold values from -3.5 to 3.5
- perf_cells: int32 [4, 32, 128], P('wells'), may hold values from 0 to 131071, as said below
- perf_count: int32 [4, 32], P('wells'), may hold values from 32 to 128
- perf_index: float32 [4, 32, 128], P('wells'), may hold values from 0.2 to 2
- seg_parent: int32 [4, 32, 32], P('wells'), may hold values from 0 to 30, as said below
- seg_cond: float32 [4, 32, 32], P('wells'), may hold values from 0.5 to 4
- seg_state: float32 [3, 4, 32, 32], P(None, 'wells'), may hold values from -6 to 6
- seg_source: float32 [3, 4, 32, 32], P(None, 'wells'), may hold values from -6 to 6
Outputs:
- cell_update: float32 [3, 4, 131072], P(None, 'wells', 'cells')
- well_update: float32 [3, 4, 32, 32], P(None, 'wells', 'cells')
- residual_max: float32 [6], replicated
The draws below stay inside these ranges and needn't reach their ends.
Inputs may be any that keep to these rules, and one draw needn't show every extreme that they name: seg_parent[..., 0] is 0; for s >= 1, seg_parent[..., s] lies between s - 3 and s - 1, so the segments of a well form a tree rooted at segment 0. `perf_cells`: in each region, take the wells in groups of 4 consecutive wells and the cells in blocks of 16384 consecutive cells; exactly 64 slots of each group, live or not, name a cell of each block.
All inputs are finite; a program needn't handle non-finite values.
Results may differ from the reference program's by a relative error of at most 0.0001.
Values sent between devices are 32-bit elements; how exact they have to be, the bound alone decides.
A program may use at most 128 MiB of HBM per device.

```python
import math
import jax
import jax.numpy as jnp

CELL_DEV = 16384
WELL_DEV = 4
P_SIZE = 128
NSEG = 32
REG = 4
RCELLS = 131072
WG = 32
N_CELLS = 8


def draw_seg_parent(key, part):
    index = jnp.arange(NSEG, dtype=jnp.int32)
    lower = jnp.maximum(index - 3, 0)
    upper = jnp.maximum(index, 1)
    lower = jnp.broadcast_to(lower, (REG, WG, NSEG))
    upper = jnp.broadcast_to(upper, (REG, WG, NSEG))
    return jax.random.randint(key, (REG, WG, NSEG), lower, upper, dtype=jnp.int32)


def draw_perf_cells(key, part):
    group_slots = WELL_DEV * P_SIZE
    groups = REG * N_CELLS
    perm_key = jax.random.fold_in(key, 11)
    offset_key = jax.random.fold_in(key, 23)
    keys = jax.random.split(perm_key, groups)
    orders = jax.vmap(lambda k: jax.random.permutation(k, group_slots))(keys).astype(jnp.int32)
    block = orders % N_CELLS
    offsets = jax.random.randint(offset_key, (groups, group_slots), 0, CELL_DEV, dtype=jnp.int32)
    cells = block * CELL_DEV + offsets
    return cells.reshape(REG, WG, P_SIZE).astype(jnp.int32)


def place_ends(drawn, key, smallest, largest):
    index_at = [jax.random.randint(jax.random.fold_in(key, axis), (), 0, length) for axis, length in enumerate(drawn.shape)]
    longest = drawn.shape.index(max(drawn.shape))
    next_to = index_at[:longest] + [(index_at[longest] + 1) % drawn.shape[longest]] + index_at[longest + 1:]
    return drawn.at[tuple(index_at)].set(smallest).at[tuple(next_to)].set(largest)


def level_of(key, extent, cuts, low, largest):
    level, own = 1.0, jax.random.fold_in(key, 6)
    for dim, parts in cuts:
        steps = jnp.exp(jax.random.uniform(jax.random.fold_in(own, dim), (parts,), jnp.float32, low / len(cuts), largest / len(cuts)))
        level = level * jnp.repeat(steps, extent[dim] // parts).reshape([-1 if axis == dim else 1 for axis in range(len(extent))])
    return level


def normal_values(rng, extent, scale, reach, cuts=(), kind=jnp.bfloat16):
    factor_of = level_of(rng, extent, cuts, -0.22, 0.18) if cuts else 1.0
    array = jax.random.normal(rng, extent, jnp.float32) * scale * factor_of
    return jnp.minimum(jnp.maximum(array, -reach), reach).astype(kind)


def setup_inputs(seed: int = 0) -> dict:
    streams_of = jax.random.split(jax.random.key(seed), 12)
    return {
        "cell_state": normal_values(streams_of[0], (3, REG, RCELLS), 1.0, 6.0, ((1, 4), (2, 8)), jnp.float32),
        "cell_residual": normal_values(streams_of[1], (3, REG, RCELLS), 1.0, 6.0, ((1, 4), (2, 8)), jnp.float32),
        "cell_block": normal_values(streams_of[2], (9, REG, RCELLS), 0.6, 4.0, ((1, 4), (2, 8)), jnp.float32),
        "block_inverse": normal_values(streams_of[3], (9, REG, RCELLS), 3 ** -0.5, 3.5, ((1, 4), (2, 8)), jnp.float32),
        "perf_cells": draw_perf_cells(jax.random.fold_in(streams_of[11], 71), 0),
        "perf_count": place_ends(jax.random.randint(streams_of[5], (REG, WG), P_SIZE // 4, P_SIZE + 1), jax.random.fold_in(streams_of[5], 1), P_SIZE // 4, P_SIZE).astype(jnp.int32),
        "perf_index": jnp.clip(jnp.exp(math.log(2.0) - 2.3025851 * jax.random.uniform(streams_of[6], (REG, WG, P_SIZE), jnp.float32) ** level_of(streams_of[6], (REG, WG, P_SIZE), ((0, 4),), -0.2, 0.2)), 0.2, 2.0),
        "seg_parent": draw_seg_parent(jax.random.fold_in(streams_of[11], 71), 0),
        "seg_cond": jnp.clip(jnp.exp(math.log(4.0) - 2.0794415 * jax.random.uniform(streams_of[8], (REG, WG, NSEG), jnp.float32) ** level_of(streams_of[8], (REG, WG, NSEG), ((0, 4),), -0.2, 0.2)), 0.5, 4.0),
        "seg_state": normal_values(streams_of[9], (3, REG, WG, NSEG), 1.0, 6.0, ((1, 4),), jnp.float32),
        "seg_source": normal_values(streams_of[10], (3, REG, WG, NSEG), 1.0, 6.0, ((1, 4),), jnp.float32),
    }


def expand_segments(values, slots):
    repeat = slots // values.shape[-1]
    wide = jnp.broadcast_to(values[..., None], values.shape + (repeat,))
    return wide.reshape(values.shape[:-1] + (slots,))

def segment_sums(values, segs):
    return jnp.sum(values.reshape(values.shape[:-1] + (segs, values.shape[-1] // segs)), axis=-1)

def perf_terms(jac_at, state_at, weight, seg_values):
    slots = weight.shape[-1]
    blocks = jac_at.reshape((3, 3) + weight.shape)
    kmat = jnp.sum(blocks[:, None] * blocks[None, :], axis=2)
    kmat = (kmat + jnp.eye(3, dtype=jnp.float32)[:, :, None, None]) * weight[None, None]
    differ = state_at - expand_segments(seg_values, slots)
    flow = jnp.sum(kmat * differ[None], axis=1)
    return (kmat, flow)

def solve_wells(ksum, rsum, parent, cond):
    segs = parent.shape[-1]
    count = parent.shape[0]
    index = jnp.arange(segs, dtype=jnp.int32)
    link = (parent[:, :, None] == index[None, None, :]) & (index[None, :, None] >= 1)
    adjacent = jnp.where(link, cond[:, :, None], jnp.float32(0.0))
    symmetric = adjacent + jnp.swapaxes(adjacent, 1, 2)
    eye_seg = jnp.eye(segs, dtype=jnp.float32)
    matrix = jnp.sum(symmetric, axis=2)[:, :, None] * eye_seg[None] - symmetric + eye_seg[None]
    eye_comp = jnp.eye(3, dtype=jnp.float32)
    blocks = jnp.transpose(ksum, (2, 3, 0, 1))
    dense = matrix[:, :, None, :, None] * eye_comp[None, None, :, None, :] + blocks[:, :, :, None, :] * eye_seg[None, :, None, :, None]
    dense = dense.reshape(count, 3 * segs, 3 * segs)
    rhs = jnp.transpose(rsum, (1, 2, 0)).reshape(count, 3 * segs)
    lower = jnp.linalg.cholesky(dense)

    def one_well(low, vec):
        return jax.scipy.linalg.cho_solve((low, True), vec)
    solved = jax.vmap(one_well)(lower, rhs)
    return jnp.transpose(solved.reshape(count, segs, 3), (2, 0, 1))

def reference(cell_state, cell_residual, cell_block, block_inverse, perf_cells, perf_count, perf_index, seg_parent, seg_cond, seg_state, seg_source):
    regions = cell_state.shape[1]
    slots = perf_cells.shape[2]
    segs = seg_parent.shape[2]
    corrected_all = []
    updates = []
    cell_tops = []
    well_tops = []
    for region in range(regions):
        index = perf_cells[region]
        live = jnp.arange(slots, dtype=jnp.int32)[None, :] < perf_count[region][:, None]
        weight = jnp.where(live, perf_index[region], jnp.float32(0.0))
        jac_at = cell_block[:, region][:, index]
        state_at = cell_state[:, region][:, index]
        kmat, flow = perf_terms(jac_at, state_at, weight, seg_state[:, region])
        ksum = segment_sums(kmat, segs)
        rsum = segment_sums(flow, segs) + seg_source[:, region]
        solved = solve_wells(ksum, rsum, seg_parent[region], seg_cond[region])
        spread = expand_segments(solved, slots)
        delta = jnp.sum(kmat * spread[None], axis=1)
        correction = jnp.zeros((3, cell_state.shape[2]), jnp.float32).at[:, index.reshape(-1)].add(delta.reshape(3, -1))
        corrected = cell_residual[:, region] - correction
        corrected_all.append(corrected)
        updates.append(solved)
        cell_tops.append(jnp.max(jnp.abs(corrected), axis=1))
        well_tops.append(jnp.max(jnp.abs(rsum), axis=(1, 2)))
    cell_top = jnp.max(jnp.stack(cell_tops), axis=0)
    well_top = jnp.max(jnp.stack(well_tops), axis=0)
    scale = 1.0 / jnp.maximum(jnp.float32(1.0), cell_top)
    steps = []
    for region in range(regions):
        inverse = block_inverse[:, region].reshape(3, 3, -1)
        steps.append(jnp.sum(inverse * corrected_all[region][None], axis=1) * scale[:, None])
    cell_update = jnp.stack(steps, axis=1)
    well_update = jnp.stack(updates, axis=1)
    residual_max = jnp.concatenate([cell_top, well_top])
    return (cell_update, well_update, residual_max)
```

```python
import functools

import jax
import jax.numpy as jnp
from jax import lax
from jax.experimental import pallas as pl
from jax.experimental.pallas import tpu as pltpu
from jax.sharding import PartitionSpec as P

MESH = pl.DeviceIdType.MESH
F32 = jnp.float32
BF16 = jnp.bfloat16
LANES = 128


def iota(shape, axis):
    return lax.broadcasted_iota(jnp.int32, shape, axis)


def split3(x):
    high = x.astype(BF16).astype(F32)
    rest = x - high
    mid = rest.astype(BF16).astype(F32)
    return high, mid, rest - mid


def dot(a, b):
    return lax.dot_general(a, b, (((1,), (0,)), ((), ())), preferred_element_type=F32)


def dot_nt(a, b):
    return lax.dot_general(a, b, (((1,), (1,)), ((), ())), preferred_element_type=F32)


def ones_where(cond):
    return jnp.where(cond, F32(1.0), F32(0.0)).astype(BF16)


def invert3(a):
    a00, a01, a02, a11, a12, a22 = a
    q0 = 1.0 / a00
    l1 = a01 * q0
    l2 = a02 * q0
    b11 = a11 - l1 * a01
    b12 = a12 - l1 * a02
    b22 = a22 - l2 * a02
    q1 = 1.0 / b11
    m = b12 * q1
    i22 = 1.0 / (b22 - m * b12)
    i12 = -m * i22
    i11 = q1 - m * i12
    i02 = -(l1 * i12 + l2 * i22)
    i01 = -(l1 * i11 + l2 * i12)
    i00 = q0 - (l1 * i01 + l2 * i02)
    return (i00, i01, i02, i11, i12, i22)


def apply3(a, v):
    a00, a01, a02, a11, a12, a22 = a
    x, y, z = v
    return (
        a00 * x + a01 * y + a02 * z,
        a01 * x + a11 * y + a12 * z,
        a02 * x + a12 * y + a22 * z,
    )


def kernel(
    ncells,
    nwells,
    state_ref,
    resid_ref,
    jac_ref,
    inv_ref,
    cells_ref,
    count_ref,
    index_ref,
    parent_ref,
    cond_ref,
    segstate_ref,
    source_ref,
    step_ref,
    well_ref,
    max_ref,
    feat_scr,
    fold_scr,
    fold_int,
    send_buf,
    recv_buf,
    top_send,
    top_recv,
    send_sem,
    recv_sem,
    top_send_sem,
    top_recv_sem,
):
    me = lax.axis_index("cells")
    region = lax.axis_index("wells")
    peers = [
        (dc, dw) for dc in range(ncells) for dw in range(nwells) if (dc, dw) != (0, 0)
    ]

    def device(dc, dw):
        return (lax.rem(me + dc, ncells), lax.rem(region + dw, nwells))

    barrier = pltpu.get_barrier_semaphore()
    for dc, dw in peers:
        pl.semaphore_signal(barrier, inc=1, device_id=device(dc, dw), device_id_type=MESH)

    wells, slots = cells_ref.shape
    segs = parent_ref.shape[1]
    rows = state_ref.shape[1]
    shard = rows * LANES
    groups = ncells
    owned = wells // groups
    per = owned * slots // ncells
    total = groups * per
    targets = owned * segs

    offset = cells_ref[...] - me * shard
    inside = (offset >= 0) & (offset < shard)
    mask = ones_where(inside)
    before = ones_where(iota((slots, slots), 0) < iota((slots, slots), 1))
    wi, wj = iota((wells, wells), 0), iota((wells, wells), 1)
    above = ones_where((wi // owned == wj // owned) & (wj < wi))
    full = jnp.ones((slots, slots), BF16)
    rank = dot(mask, before) + dot(dot(above, mask).astype(BF16), full)
    rank = jnp.where(inside, rank, F32(-1.0))
    counts = dot(
        jnp.where(wi == wj, count_ref[...].astype(F32), F32(0.0)).astype(BF16),
        jnp.ones((wells, slots), BF16),
    )
    live = iota((wells, slots), 1).astype(F32) < counts
    weight = jnp.where(live, index_ref[...], F32(0.0))
    hi = jnp.where(inside, offset // LANES, 0).astype(F32)
    lo = jnp.where(inside, offset % LANES, 0).astype(F32)
    slot_seg = iota((1, slots), 1) // (slots // segs)
    parts = (hi, lo) + split3(weight)
    sub = iota((8, slots), 0)
    order = iota((per, slots), 0).astype(F32)
    for g in range(groups):
        feats, picks = [], []
        for j in range(owned):
            w = g * owned + j
            f = jnp.broadcast_to((slot_seg + j * segs).astype(F32), (8, slots))
            for k, part in enumerate(parts):
                f = jnp.where(sub == k, part[w : w + 1], f)
            feats.append(f)
            picks.append(ones_where(rank[w : w + 1] == order))
        feat_scr[:, g * per : (g + 1) * per] = dot_nt(
            jnp.concatenate(feats, axis=1).astype(BF16), jnp.concatenate(picks, axis=1)
        )

    slot_hi = feat_scr[0:1]
    slot_lo = feat_scr[1:2]
    slot_weight = feat_scr[2:3] + feat_scr[3:4] + feat_scr[4:5]
    slot_target = feat_scr[5:6]
    at_lo = ones_where(iota((LANES, total), 0).astype(F32) == slot_lo)
    at_hi = iota((rows, total), 0).astype(F32) == slot_hi
    at_target = ones_where(iota((targets, total), 0).astype(F32) == slot_target)
    in_group = iota((groups, total), 1) // per == iota((groups, total), 0)
    at_lo3 = jnp.concatenate([at_lo] * 3, axis=0)

    def cell_values(values):
        pieces = jnp.concatenate([p.astype(BF16) for p in split3(values)], axis=1)
        spread = dot(pieces, at_lo3)
        return jnp.sum(jnp.where(at_hi, spread, F32(0.0)), axis=0, keepdims=True)

    def table_values(tables):
        pieces = [split3(t) for t in tables]
        stacked = jnp.concatenate([p[i] for i in range(3) for p in pieces], axis=0)
        spread = dot(stacked.astype(BF16), at_target)
        size = len(tables) * groups
        spread = spread[:size] + spread[size : 2 * size] + spread[2 * size :]
        return [
            jnp.sum(
                jnp.where(in_group, spread[k * groups : (k + 1) * groups], F32(0.0)),
                axis=0,
                keepdims=True,
            )
            for k in range(len(tables))
        ]

    def fold(read, scratch):
        for j in range(owned):
            scratch[:, j * segs : (j + 1) * segs] = read(pl.ds(j, groups, stride=owned))
        return scratch[...]

    seg_state = [
        fold(lambda s, k=k: segstate_ref[k, s, :], fold_scr.at[k]) for k in range(3)
    ]
    source = [fold(lambda s, k=k: source_ref[k, s, :], fold_scr.at[3 + k]) for k in range(3)]
    cond = fold(lambda s: cond_ref[s, :], fold_scr.at[6])
    parent = fold(lambda s: parent_ref[s, :], fold_int)

    state_at = [cell_values(state_ref[k]) for k in range(3)]
    jac = [cell_values(jac_ref[k]) for k in range(9)]
    differ = [a - b for a, b in zip(state_at, table_values(seg_state))]
    kmat = []
    for a in range(3):
        for b in range(a, 3):
            entry = sum(jac[3 * a + c] * jac[3 * b + c] for c in range(3))
            kmat.append((entry + 1.0 if a == b else entry) * slot_weight)
    flow = apply3(kmat, differ)
    values = [split3(v) for v in kmat + list(flow)]
    placed = jnp.concatenate(
        [jnp.where(in_group, v[i], F32(0.0)) for i in range(3) for v in values], axis=0
    )
    summed = dot_nt(placed.astype(BF16), at_target)
    size = 9 * groups
    send_buf[...] = summed[:size] + summed[size : 2 * size] + summed[2 * size :]

    pl.semaphore_wait(barrier, len(peers))
    copies = []
    for d in range(1, ncells):
        copy = pltpu.make_async_remote_copy(
            src_ref=send_buf,
            dst_ref=recv_buf.at[d - 1],
            send_sem=send_sem.at[d - 1],
            recv_sem=recv_sem.at[d - 1],
            device_id=device(d, 0),
            device_id_type=MESH,
        )
        copy.start()
        copies.append(copy)

    seg = iota((groups, targets), 1) % segs
    dist = seg - parent
    links = [jnp.where((dist == d) & (seg >= 1), cond, F32(0.0)) for d in (1, 2, 3)]

    def roll(x, shift):
        shift = shift % targets
        return pltpu.roll(x, shift, 1) if shift else x

    diagonal = 1.0 + links[0] + links[1] + links[2]
    for d in (1, 2, 3):
        diagonal = diagonal + roll(links[d - 1], -d)

    table = send_buf[...]
    for copy in copies:
        copy.wait_recv()
    for d in range(1, ncells):
        table = table + recv_buf[d - 1]
    table = [table[k * groups : (k + 1) * groups] for k in range(9)]
    for k in (0, 3, 5):
        table[k] = table[k] + diagonal
    for k in range(3):
        table[6 + k] = table[6 + k] + source[k]
    well_top = [jnp.max(jnp.abs(table[6 + k])) for k in range(3)]

    mats = [[roll(table[k], -s) for k in range(6)] for s in range(segs)]
    vecs = [[roll(table[6 + k], -s) for k in range(3)] for s in range(segs)]
    edges = [[roll(link, -s) for link in links] for s in range(segs)]
    inverses, partial = [None] * segs, [None] * segs
    for s in range(segs - 1, -1, -1):
        inverses[s] = invert3(mats[s])
        partial[s] = apply3(inverses[s], vecs[s])
        for d in (1, 2, 3):
            if s - d >= 0:
                c = edges[s][d - 1]
                c2 = c * c
                mats[s - d] = [a - c2 * i for a, i in zip(mats[s - d], inverses[s])]
                vecs[s - d] = [r + c * y for r, y in zip(vecs[s - d], partial[s])]
    found = [partial[0]]
    for s in range(1, segs):
        pull = [
            sum(edges[s][d - 1] * found[s - d][k] for d in (1, 2, 3) if s - d >= 0)
            for k in range(3)
        ]
        found.append([y + x for y, x in zip(partial[s], apply3(inverses[s], pull))])
    solved = []
    for k in range(3):
        out = found[0][k]
        for s in range(1, segs):
            out = jnp.where(seg == s, roll(found[s][k], s), out)
        solved.append(out)

    mine = iota((groups, targets), 0) == me
    for k in range(3):
        row = jnp.sum(jnp.where(mine, solved[k], F32(0.0)), axis=0, keepdims=True)
        for j in range(owned):
            well_ref[k, j : j + 1, :] = row[:, j * segs : (j + 1) * segs]

    delta = apply3(kmat, table_values(solved))
    at_lo_wide = jnp.concatenate([at_lo] * 3, axis=1)
    corrected, tops = [], []
    for k in range(3):
        spread = jnp.concatenate(
            [jnp.where(at_hi, p, F32(0.0)).astype(BF16) for p in split3(delta[k])], axis=1
        )
        fixed = resid_ref[k] - dot_nt(spread, at_lo_wide)
        corrected.append(fixed)
        tops.append(jnp.max(jnp.abs(fixed)))
    tops = tops + well_top

    lane = iota((1, LANES), 1)
    top = jnp.zeros((1, LANES), F32)
    for k in range(6):
        top = jnp.where(lane == k, tops[k], top)
    top_send[...] = top
    sends = []
    for i, (dc, dw) in enumerate(peers):
        copy = pltpu.make_async_remote_copy(
            src_ref=top_send,
            dst_ref=top_recv.at[i],
            send_sem=top_send_sem,
            recv_sem=top_recv_sem,
            device_id=device(dc, dw),
            device_id_type=MESH,
        )
        copy.start()
    steps = []
    for a in range(3):
        steps.append(sum(inv_ref[3 * a + b] * corrected[b] for b in range(3)))
    pltpu.make_async_copy(top_recv, top_recv, top_recv_sem).wait()
    top = jnp.maximum(top, jnp.max(top_recv[...], axis=0))
    scale = 1.0 / jnp.maximum(F32(1.0), top)
    for k in range(3):
        step_ref[k] = steps[k] * scale[:, k : k + 1]
    for k in range(6):
        max_ref[k] = jnp.max(jnp.where(lane == k, top, F32(0.0)))
    for copy in copies:
        copy.wait_send()
    pltpu.make_async_copy(top_recv, top_recv, top_send_sem).wait()


def on_device(ncells, nwells, *args):
    (
        cell_state,
        cell_residual,
        cell_block,
        block_inverse,
        perf_cells,
        perf_count,
        perf_index,
        seg_parent,
        seg_cond,
        seg_state,
        seg_source,
    ) = args
    shard = cell_state.shape[2]
    rows = shard // LANES
    wells, slots = perf_cells.shape[1:]
    segs = seg_parent.shape[2]
    owned = wells // ncells
    total = owned * slots
    targets = owned * segs
    others = ncells * nwells - 1

    def planes(x):
        return x.reshape(x.shape[0], rows, LANES)

    vmem = pl.BlockSpec(memory_space=pltpu.VMEM)
    step, well, top = pl.pallas_call(
        functools.partial(kernel, ncells, nwells),
        out_shape=(
            jax.ShapeDtypeStruct((3, rows, LANES), F32),
            jax.ShapeDtypeStruct((3, owned, segs), F32),
            jax.ShapeDtypeStruct((6,), F32),
        ),
        in_specs=[vmem] * 11,
        out_specs=(vmem, vmem, pl.BlockSpec(memory_space=pltpu.SMEM)),
        scratch_shapes=[
            pltpu.VMEM((8, total), F32),
            pltpu.VMEM((7, ncells, targets), F32),
            pltpu.VMEM((ncells, targets), jnp.int32),
            pltpu.VMEM((9 * ncells, targets), F32),
            pltpu.VMEM((ncells - 1, 9 * ncells, targets), F32),
            pltpu.VMEM((1, LANES), F32),
            pltpu.VMEM((others, 1, LANES), F32),
            pltpu.SemaphoreType.DMA((ncells - 1,)),
            pltpu.SemaphoreType.DMA((ncells - 1,)),
            pltpu.SemaphoreType.DMA,
            pltpu.SemaphoreType.DMA,
        ],
        compiler_params=pltpu.CompilerParams(collective_id=0, has_side_effects=True),
    )(
        planes(cell_state),
        planes(cell_residual),
        planes(cell_block),
        planes(block_inverse),
        perf_cells[0],
        perf_count,
        perf_index[0],
        seg_parent[0],
        seg_cond[0],
        seg_state[:, 0],
        seg_source[:, 0],
    )
    return (step.reshape(3, 1, shard), well[:, None], top)


def solution(mesh):
    in_specs = (
        P(None, "wells", "cells"),
        P(None, "wells", "cells"),
        P(None, "wells", "cells"),
        P(None, "wells", "cells"),
        P("wells", None, None),
        P("wells", None),
        P("wells", None, None),
        P("wells", None, None),
        P("wells", None, None),
        P(None, "wells", None, None),
        P(None, "wells", None, None),
    )
    out_specs = (P(None, "wells", "cells"), P(None, "wells", "cells", None), P())
    return jax.shard_map(
        functools.partial(on_device, mesh.shape["cells"], mesh.shape["wells"]),
        mesh=mesh,
        in_specs=in_specs,
        out_specs=out_specs,
        check_vma=False,
    )
```

```python
import functools

import jax
import jax.numpy as jnp
from jax import lax
from jax.experimental import pallas as pl
from jax.experimental.pallas import tpu as pltpu
from jax.sharding import PartitionSpec as P

MESH = pl.DeviceIdType.MESH
F32 = jnp.float32
BF16 = jnp.bfloat16
LANES = 128


def iota(shape, axis):
    return lax.broadcasted_iota(jnp.int32, shape, axis)


def split3(x):
    high = x.astype(BF16).astype(F32)
    rest = x - high
    mid = rest.astype(BF16).astype(F32)
    return high, mid, rest - mid


def dot(a, b):
    return lax.dot_general(a, b, (((1,), (0,)), ((), ())), preferred_element_type=F32)


def dot_nt(a, b):
    return lax.dot_general(a, b, (((1,), (1,)), ((), ())), preferred_element_type=F32)


def ones_where(cond):
    return jnp.where(cond, F32(1.0), F32(0.0)).astype(BF16)


def invert3(a):
    a00, a01, a02, a11, a12, a22 = a
    q0 = 1.0 / a00
    l1 = a01 * q0
    l2 = a02 * q0
    b11 = a11 - l1 * a01
    b12 = a12 - l1 * a02
    b22 = a22 - l2 * a02
    q1 = 1.0 / b11
    m = b12 * q1
    i22 = 1.0 / (b22 - m * b12)
    i12 = -m * i22
    i11 = q1 - m * i12
    i02 = -(l1 * i12 + l2 * i22)
    i01 = -(l1 * i11 + l2 * i12)
    i00 = q0 - (l1 * i01 + l2 * i02)
    return (i00, i01, i02, i11, i12, i22)


def apply3(a, v):
    a00, a01, a02, a11, a12, a22 = a
    x, y, z = v
    return (
        a00 * x + a01 * y + a02 * z,
        a01 * x + a11 * y + a12 * z,
        a02 * x + a12 * y + a22 * z,
    )


def kernel(
    ncells,
    nwells,
    state_hbm,
    jac_hbm,
    resid_hbm,
    inv_hbm,
    cells_ref,
    count_ref,
    index_ref,
    parent_ref,
    cond_ref,
    segstate_ref,
    source_ref,
    step_ref,
    well_ref,
    top_ref,
    state_ref,
    jac_ref,
    resid_ref,
    inv_ref,
    load_sem,
    feat_scr,
    fold_scr,
    fold_int,
    send_buf,
    recv_buf,
    top_send,
    top_recv,
    send_sem,
    recv_sem,
    top_send_sem,
    top_recv_sem,
):
    loads = [
        pltpu.make_async_copy(src, dst, load_sem.at[i])
        for i, (src, dst) in enumerate(
            (
                (state_hbm, state_ref),
                (jac_hbm, jac_ref),
                (resid_hbm, resid_ref),
                (inv_hbm, inv_ref),
            )
        )
    ]
    for load in loads:
        load.start()
    me = lax.axis_index("cells")
    region = lax.axis_index("wells")
    peers = [
        (dc, dw) for dc in range(ncells) for dw in range(nwells) if (dc, dw) != (0, 0)
    ]

    def device(dc, dw):
        return (lax.rem(me + dc, ncells), lax.rem(region + dw, nwells))

    barrier = pltpu.get_barrier_semaphore()
    greeted = [(dc, dw) for dc, dw in peers if dc == 0 or dw == 0]
    for dc, dw in greeted:
        pl.semaphore_signal(barrier, inc=1, device_id=device(dc, dw), device_id_type=MESH)

    wells, slots = cells_ref.shape
    segs = parent_ref.shape[1]
    rows = state_ref.shape[1]
    shard = rows * LANES
    groups = ncells
    owned = wells // groups
    per = owned * slots // ncells
    total = groups * per
    targets = owned * segs

    offset = cells_ref[...] - me * shard
    inside = (offset >= 0) & (offset < shard)
    mask = ones_where(inside)
    before = ones_where(iota((slots, slots), 0) < iota((slots, slots), 1))
    wi, wj = iota((wells, wells), 0), iota((wells, wells), 1)
    above = ones_where((wi // owned == wj // owned) & (wj < wi))
    full = jnp.ones((slots, slots), BF16)
    rank = dot(mask, before) + dot(dot(above, mask).astype(BF16), full)
    rank = jnp.where(inside, rank, F32(-1.0))
    counts = dot(
        jnp.where(wi == wj, count_ref[...].astype(F32), F32(0.0)).astype(BF16),
        jnp.ones((wells, slots), BF16),
    )
    live = iota((wells, slots), 1).astype(F32) < counts
    weight = jnp.where(live, index_ref[...], F32(0.0))
    hi = jnp.where(inside, offset // LANES, 0).astype(F32)
    lo = jnp.where(inside, offset % LANES, 0).astype(F32)
    slot_seg = iota((1, slots), 1) // (slots // segs)
    parts = (hi, lo) + split3(weight)
    sub = iota((8, slots), 0)
    order = iota((per, slots), 0).astype(F32)
    for g in range(groups):
        feats, picks = [], []
        for j in range(owned):
            w = g * owned + j
            f = jnp.broadcast_to((slot_seg + j * segs).astype(F32), (8, slots))
            for k, part in enumerate(parts):
                f = jnp.where(sub == k, part[w : w + 1], f)
            feats.append(f)
            picks.append(ones_where(rank[w : w + 1] == order))
        feat_scr[:, g * per : (g + 1) * per] = dot_nt(
            jnp.concatenate(feats, axis=1).astype(BF16), jnp.concatenate(picks, axis=1)
        )

    slot_hi = feat_scr[0:1]
    slot_lo = feat_scr[1:2]
    slot_weight = feat_scr[2:3] + feat_scr[3:4] + feat_scr[4:5]
    slot_target = feat_scr[5:6]
    at_lo = ones_where(iota((LANES, total), 0).astype(F32) == slot_lo)
    at_hi = iota((rows, total), 0).astype(F32) == slot_hi
    at_target = ones_where(iota((targets, total), 0).astype(F32) == slot_target)
    in_group = iota((groups, total), 1) // per == iota((groups, total), 0)
    at_lo3 = jnp.concatenate([at_lo] * 3, axis=0)

    def cell_values(values):
        pieces = jnp.concatenate([p.astype(BF16) for p in split3(values)], axis=1)
        spread = dot(pieces, at_lo3)
        return jnp.sum(jnp.where(at_hi, spread, F32(0.0)), axis=0, keepdims=True)

    def table_values(tables):
        pieces = [split3(t) for t in tables]
        stacked = jnp.concatenate([p[i] for i in range(3) for p in pieces], axis=0)
        spread = dot(stacked.astype(BF16), at_target)
        size = len(tables) * groups
        spread = spread[:size] + spread[size : 2 * size] + spread[2 * size :]
        return [
            jnp.sum(
                jnp.where(in_group, spread[k * groups : (k + 1) * groups], F32(0.0)),
                axis=0,
                keepdims=True,
            )
            for k in range(len(tables))
        ]

    def fold(read, scratch):
        for j in range(owned):
            scratch[:, j * segs : (j + 1) * segs] = read(pl.ds(j, groups, stride=owned))
        return scratch[...]

    seg_state = [
        fold(lambda s, k=k: segstate_ref[k, s, :], fold_scr.at[k]) for k in range(3)
    ]
    source = [fold(lambda s, k=k: source_ref[k, s, :], fold_scr.at[3 + k]) for k in range(3)]
    cond = fold(lambda s: cond_ref[s, :], fold_scr.at[6])
    parent = fold(lambda s: parent_ref[s, :], fold_int)

    loads[0].wait()
    loads[1].wait()
    state_at = [cell_values(state_ref[k]) for k in range(3)]
    jac = [cell_values(jac_ref[k]) for k in range(9)]
    differ = [a - b for a, b in zip(state_at, table_values(seg_state))]
    kmat = []
    for a in range(3):
        for b in range(a, 3):
            entry = sum(jac[3 * a + c] * jac[3 * b + c] for c in range(3))
            kmat.append((entry + 1.0 if a == b else entry) * slot_weight)
    flow = apply3(kmat, differ)
    values = [split3(v) for v in kmat + list(flow)]
    placed = jnp.concatenate(
        [jnp.where(in_group, v[i], F32(0.0)) for i in range(3) for v in values], axis=0
    )
    summed = dot_nt(placed.astype(BF16), at_target)
    size = 9 * groups
    send_buf[...] = summed[:size] + summed[size : 2 * size] + summed[2 * size :]

    pl.semaphore_wait(barrier, len(greeted))
    copies = []
    for d in range(1, ncells):
        copy = pltpu.make_async_remote_copy(
            src_ref=send_buf,
            dst_ref=recv_buf.at[d - 1],
            send_sem=send_sem.at[d - 1],
            recv_sem=recv_sem.at[d - 1],
            device_id=device(d, 0),
            device_id_type=MESH,
        )
        copy.start()
        copies.append(copy)

    seg = iota((groups, targets), 1) % segs
    dist = seg - parent
    links = [jnp.where((dist == d) & (seg >= 1), cond, F32(0.0)) for d in (1, 2, 3)]

    def roll(x, shift):
        shift = shift % targets
        return pltpu.roll(x, shift, 1) if shift else x

    diagonal = 1.0 + links[0] + links[1] + links[2]
    for d in (1, 2, 3):
        diagonal = diagonal + roll(links[d - 1], -d)

    edges = [[roll(link, -s) for link in links] for s in range(segs)]
    at_lo_wide = jnp.concatenate([at_lo] * 3, axis=1)
    loads[2].wait()
    loads[3].wait()

    table = send_buf[...]
    for copy in copies:
        copy.wait_recv()
    for d in range(1, ncells):
        table = table + recv_buf[d - 1]
    table = [table[k * groups : (k + 1) * groups] for k in range(9)]
    for k in (0, 3, 5):
        table[k] = table[k] + diagonal
    for k in range(3):
        table[6 + k] = table[6 + k] + source[k]
    well_top = [jnp.max(jnp.abs(table[6 + k])) for k in range(3)]

    mats = [[roll(table[k], -s) for k in range(6)] for s in range(segs)]
    vecs = [[roll(table[6 + k], -s) for k in range(3)] for s in range(segs)]
    inverses, partial = [None] * segs, [None] * segs
    for s in range(segs - 1, -1, -1):
        inverses[s] = invert3(mats[s])
        partial[s] = apply3(inverses[s], vecs[s])
        for d in (1, 2, 3):
            if s - d >= 0:
                c = edges[s][d - 1]
                c2 = c * c
                mats[s - d] = [a - c2 * i for a, i in zip(mats[s - d], inverses[s])]
                vecs[s - d] = [r + c * y for r, y in zip(vecs[s - d], partial[s])]
    found = [partial[0]]
    for s in range(1, segs):
        pull = [
            sum(edges[s][d - 1] * found[s - d][k] for d in (1, 2, 3) if s - d >= 0)
            for k in range(3)
        ]
        found.append([y + x for y, x in zip(partial[s], apply3(inverses[s], pull))])
    solved = []
    for k in range(3):
        out = found[0][k]
        for s in range(1, segs):
            out = jnp.where(seg == s, roll(found[s][k], s), out)
        solved.append(out)

    mine = iota((groups, targets), 0) == me
    for k in range(3):
        row = jnp.sum(jnp.where(mine, solved[k], F32(0.0)), axis=0, keepdims=True)
        for j in range(owned):
            well_ref[k, j : j + 1, :] = row[:, j * segs : (j + 1) * segs]

    delta = apply3(kmat, table_values(solved))
    corrected, tops = [], []
    for k in range(3):
        spread = jnp.concatenate(
            [jnp.where(at_hi, p, F32(0.0)).astype(BF16) for p in split3(delta[k])], axis=1
        )
        fixed = resid_ref[k] - dot_nt(spread, at_lo_wide)
        corrected.append(fixed)
        tops.append(jnp.max(jnp.abs(fixed)))
    tops = tops + well_top

    lane = iota((1, LANES), 1)
    top = jnp.zeros((1, LANES), F32)
    for k in range(6):
        top = jnp.where(lane == k, tops[k], top)
    top_send[...] = top
    sends = []
    for i, (dc, dw) in enumerate(peers):
        copy = pltpu.make_async_remote_copy(
            src_ref=top_send,
            dst_ref=top_recv.at[i],
            send_sem=top_send_sem,
            recv_sem=top_recv_sem,
            device_id=device(dc, dw),
            device_id_type=MESH,
        )
        copy.start()
    for a in range(3):
        step_ref[a] = sum(inv_ref[3 * a + b] * corrected[b] for b in range(3))
    pltpu.make_async_copy(top_recv, top_recv, top_recv_sem).wait()
    top = jnp.maximum(top, jnp.max(top_recv[...], axis=0))
    top_ref[...] = top
    for copy in copies:
        copy.wait_send()
    pltpu.make_async_copy(top_recv, top_recv, top_send_sem).wait()


def finish(step_in, well_in, top_in, step_ref, well_ref, max_ref):
    top = top_in[...]
    scale = 1.0 / jnp.maximum(F32(1.0), top)
    for k in range(3):
        step_ref[k] = step_in[k] * scale[:, k : k + 1]
    well_ref[...] = well_in[...]
    lane = iota(top.shape, 1)
    for k in range(6):
        max_ref[k] = jnp.max(jnp.where(lane == k, top, F32(0.0)))


def on_device(ncells, nwells, *args):
    (
        cell_state,
        cell_residual,
        cell_block,
        block_inverse,
        perf_cells,
        perf_count,
        perf_index,
        seg_parent,
        seg_cond,
        seg_state,
        seg_source,
    ) = args
    shard = cell_state.shape[2]
    rows = shard // LANES
    wells, slots = perf_cells.shape[1:]
    segs = seg_parent.shape[2]
    owned = wells // ncells
    total = owned * slots
    targets = owned * segs
    others = ncells * nwells - 1

    def planes(x):
        return x.reshape(x.shape[0], rows, LANES)

    vmem = pl.BlockSpec(memory_space=pltpu.VMEM)
    hbm = pl.BlockSpec(memory_space=pltpu.HBM)
    raw, found, top = pl.pallas_call(
        functools.partial(kernel, ncells, nwells),
        out_shape=(
            jax.ShapeDtypeStruct((3, rows, LANES), F32),
            jax.ShapeDtypeStruct((3, owned, segs), F32),
            jax.ShapeDtypeStruct((1, LANES), F32),
        ),
        in_specs=[hbm] * 4 + [vmem] * 7,
        out_specs=(vmem, vmem, vmem),
        scratch_shapes=[
            pltpu.VMEM((3, rows, LANES), F32),
            pltpu.VMEM((9, rows, LANES), F32),
            pltpu.VMEM((3, rows, LANES), F32),
            pltpu.VMEM((9, rows, LANES), F32),
            pltpu.SemaphoreType.DMA((4,)),
            pltpu.VMEM((8, total), F32),
            pltpu.VMEM((7, ncells, targets), F32),
            pltpu.VMEM((ncells, targets), jnp.int32),
            pltpu.VMEM((9 * ncells, targets), F32),
            pltpu.VMEM((ncells - 1, 9 * ncells, targets), F32),
            pltpu.VMEM((1, LANES), F32),
            pltpu.VMEM((others, 1, LANES), F32),
            pltpu.SemaphoreType.DMA((ncells - 1,)),
            pltpu.SemaphoreType.DMA((ncells - 1,)),
            pltpu.SemaphoreType.DMA,
            pltpu.SemaphoreType.DMA,
        ],
        compiler_params=pltpu.CompilerParams(collective_id=0, has_side_effects=True),
    )(
        planes(cell_state),
        planes(cell_block),
        planes(cell_residual),
        planes(block_inverse),
        perf_cells[0],
        perf_count,
        perf_index[0],
        seg_parent[0],
        seg_cond[0],
        seg_state[:, 0],
        seg_source[:, 0],
    )
    step, well, top = pl.pallas_call(
        finish,
        out_shape=(
            jax.ShapeDtypeStruct((3, rows, LANES), F32),
            jax.ShapeDtypeStruct((3, owned, segs), F32),
            jax.ShapeDtypeStruct((6,), F32),
        ),
        in_specs=[vmem] * 3,
        out_specs=(vmem, vmem, pl.BlockSpec(memory_space=pltpu.SMEM)),
    )(raw, found, top)
    return (step.reshape(3, 1, shard), well[:, None], top)


def solution(mesh):
    in_specs = (
        P(None, "wells", "cells"),
        P(None, "wells", "cells"),
        P(None, "wells", "cells"),
        P(None, "wells", "cells"),
        P("wells", None, None),
        P("wells", None),
        P("wells", None, None),
        P("wells", None, None),
        P("wells", None, None),
        P(None, "wells", None, None),
        P(None, "wells", None, None),
    )
    out_specs = (P(None, "wells", "cells"), P(None, "wells", "cells", None), P())
    return jax.shard_map(
        functools.partial(on_device, mesh.shape["cells"], mesh.shape["wells"]),
        mesh=mesh,
        in_specs=in_specs,
        out_specs=out_specs,
        check_vma=False,
    )
```

```python
import functools

import jax
import jax.numpy as jnp
from jax import lax
from jax.experimental import pallas as pl
from jax.experimental.pallas import tpu as pltpu
from jax.sharding import PartitionSpec as P

MESH = pl.DeviceIdType.MESH
F32 = jnp.float32
BF16 = jnp.bfloat16
LANES = 128


def iota(shape, axis):
    return lax.broadcasted_iota(jnp.int32, shape, axis)


def split3(x):
    high = x.astype(BF16).astype(F32)
    rest = x - high
    mid = rest.astype(BF16).astype(F32)
    return high, mid, rest - mid


def dot(a, b):
    return lax.dot_general(a, b, (((1,), (0,)), ((), ())), preferred_element_type=F32)


def dot_nt(a, b):
    return lax.dot_general(a, b, (((1,), (1,)), ((), ())), preferred_element_type=F32)


def ones_where(cond):
    return jnp.where(cond, F32(1.0), F32(0.0)).astype(BF16)


def invert3(a):
    a00, a01, a02, a11, a12, a22 = a
    q0 = 1.0 / a00
    l1 = a01 * q0
    l2 = a02 * q0
    b11 = a11 - l1 * a01
    b12 = a12 - l1 * a02
    b22 = a22 - l2 * a02
    q1 = 1.0 / b11
    m = b12 * q1
    i22 = 1.0 / (b22 - m * b12)
    i12 = -m * i22
    i11 = q1 - m * i12
    i02 = -(l1 * i12 + l2 * i22)
    i01 = -(l1 * i11 + l2 * i12)
    i00 = q0 - (l1 * i01 + l2 * i02)
    return (i00, i01, i02, i11, i12, i22)


def apply3(a, v):
    a00, a01, a02, a11, a12, a22 = a
    x, y, z = v
    return (
        a00 * x + a01 * y + a02 * z,
        a01 * x + a11 * y + a12 * z,
        a02 * x + a12 * y + a22 * z,
    )


def kernel(
    ncells,
    nwells,
    state_hbm,
    jac_hbm,
    resid_hbm,
    inv_hbm,
    cells_ref,
    count_ref,
    index_ref,
    parent_ref,
    cond_ref,
    segstate_ref,
    source_ref,
    step_ref,
    well_ref,
    top_ref,
    state_ref,
    jac_ref,
    resid_ref,
    inv_ref,
    load_sem,
    feat_scr,
    fold_scr,
    fold_int,
    send_buf,
    recv_buf,
    top_send,
    top_recv,
    send_sem,
    recv_sem,
    top_send_sem,
    top_recv_sem,
):
    loads = [
        pltpu.make_async_copy(src, dst, load_sem.at[i])
        for i, (src, dst) in enumerate(
            (
                (state_hbm, state_ref),
                (jac_hbm, jac_ref),
                (resid_hbm, resid_ref),
                (inv_hbm, inv_ref),
            )
        )
    ]
    for load in loads:
        load.start()
    me = lax.axis_index("cells")
    region = lax.axis_index("wells")
    peers = [
        (dc, dw) for dc in range(ncells) for dw in range(nwells) if (dc, dw) != (0, 0)
    ]

    def device(dc, dw):
        return (lax.rem(me + dc, ncells), lax.rem(region + dw, nwells))

    barrier = pltpu.get_barrier_semaphore()
    greeted = [(dc, dw) for dc, dw in peers if dc == 0 or dw == 0]
    for dc, dw in greeted:
        pl.semaphore_signal(barrier, inc=1, device_id=device(dc, dw), device_id_type=MESH)

    wells, slots = cells_ref.shape
    segs = parent_ref.shape[1]
    rows = state_ref.shape[1]
    shard = rows * LANES
    groups = ncells
    owned = wells // groups
    per = owned * slots // ncells
    total = groups * per
    targets = owned * segs

    offset = cells_ref[...] - me * shard
    inside = (offset >= 0) & (offset < shard)
    mask = ones_where(inside)
    before = ones_where(iota((slots, slots), 0) < iota((slots, slots), 1))
    wi, wj = iota((wells, wells), 0), iota((wells, wells), 1)
    above = ones_where((wi // owned == wj // owned) & (wj < wi))
    full = jnp.ones((slots, slots), BF16)
    rank = dot(mask, before) + dot(dot(above, mask).astype(BF16), full)
    rank = jnp.where(inside, rank, F32(-1.0))
    counts = dot(
        jnp.where(wi == wj, count_ref[...].astype(F32), F32(0.0)).astype(BF16),
        jnp.ones((wells, slots), BF16),
    )
    live = iota((wells, slots), 1).astype(F32) < counts
    weight = jnp.where(live, index_ref[...], F32(0.0))
    hi = jnp.where(inside, offset // LANES, 0).astype(F32)
    lo = jnp.where(inside, offset % LANES, 0).astype(F32)
    slot_seg = iota((1, slots), 1) // (slots // segs)
    parts = (hi, lo) + split3(weight)
    sub = iota((8, slots), 0)
    order = iota((per, slots), 0).astype(F32)
    for g in range(groups):
        feats, picks = [], []
        for j in range(owned):
            w = g * owned + j
            f = jnp.broadcast_to((slot_seg + j * segs).astype(F32), (8, slots))
            for k, part in enumerate(parts):
                f = jnp.where(sub == k, part[w : w + 1], f)
            feats.append(f)
            picks.append(ones_where(rank[w : w + 1] == order))
        feat_scr[:, g * per : (g + 1) * per] = dot_nt(
            jnp.concatenate(feats, axis=1).astype(BF16), jnp.concatenate(picks, axis=1)
        )

    slot_hi = feat_scr[0:1]
    slot_lo = feat_scr[1:2]
    slot_weight = feat_scr[2:3] + feat_scr[3:4] + feat_scr[4:5]
    slot_target = feat_scr[5:6]
    at_lo = ones_where(iota((LANES, total), 0).astype(F32) == slot_lo)
    at_hi = iota((rows, total), 0).astype(F32) == slot_hi
    at_target = ones_where(iota((targets, total), 0).astype(F32) == slot_target)
    in_group = iota((groups, total), 1) // per == iota((groups, total), 0)
    at_lo3 = jnp.concatenate([at_lo] * 3, axis=0)

    def cell_values(values):
        pieces = jnp.concatenate([p.astype(BF16) for p in split3(values)], axis=1)
        spread = dot(pieces, at_lo3)
        return jnp.sum(jnp.where(at_hi, spread, F32(0.0)), axis=0, keepdims=True)

    def table_values(tables):
        pieces = [split3(t) for t in tables]
        stacked = jnp.concatenate([p[i] for i in range(3) for p in pieces], axis=0)
        spread = dot(stacked.astype(BF16), at_target)
        size = len(tables) * groups
        spread = spread[:size] + spread[size : 2 * size] + spread[2 * size :]
        return [
            jnp.sum(
                jnp.where(in_group, spread[k * groups : (k + 1) * groups], F32(0.0)),
                axis=0,
                keepdims=True,
            )
            for k in range(len(tables))
        ]

    def fold(read, scratch):
        for j in range(owned):
            scratch[:, j * segs : (j + 1) * segs] = read(pl.ds(j, groups, stride=owned))
        return scratch[...]

    seg_state = [
        fold(lambda s, k=k: segstate_ref[k, s, :], fold_scr.at[k]) for k in range(3)
    ]
    source = [fold(lambda s, k=k: source_ref[k, s, :], fold_scr.at[3 + k]) for k in range(3)]
    cond = fold(lambda s: cond_ref[s, :], fold_scr.at[6])
    parent = fold(lambda s: parent_ref[s, :], fold_int)

    loads[0].wait()
    loads[1].wait()
    state_at = [cell_values(state_ref[k]) for k in range(3)]
    jac = [cell_values(jac_ref[k]) for k in range(9)]
    differ = [a - b for a, b in zip(state_at, table_values(seg_state))]
    kmat = []
    for a in range(3):
        for b in range(a, 3):
            entry = sum(jac[3 * a + c] * jac[3 * b + c] for c in range(3))
            kmat.append((entry + 1.0 if a == b else entry) * slot_weight)
    flow = apply3(kmat, differ)
    values = [split3(v) for v in kmat + list(flow)]
    placed = jnp.concatenate(
        [jnp.where(in_group, v[i], F32(0.0)) for i in range(3) for v in values], axis=0
    )
    summed = dot_nt(placed.astype(BF16), at_target)
    size = 9 * groups
    send_buf[...] = summed[:size] + summed[size : 2 * size] + summed[2 * size :]

    pl.semaphore_wait(barrier, len(greeted))
    copies = []
    for d in range(1, ncells):
        copy = pltpu.make_async_remote_copy(
            src_ref=send_buf,
            dst_ref=recv_buf.at[d - 1],
            send_sem=send_sem.at[d - 1],
            recv_sem=recv_sem.at[d - 1],
            device_id=device(d, 0),
            device_id_type=MESH,
        )
        copy.start()
        copies.append(copy)

    seg = iota((groups, targets), 1) % segs
    dist = seg - parent
    links = [jnp.where((dist == d) & (seg >= 1), cond, F32(0.0)) for d in (1, 2, 3)]

    def roll(x, shift):
        shift = shift % targets
        return pltpu.roll(x, shift, 1) if shift else x

    diagonal = 1.0 + links[0] + links[1] + links[2]
    for d in (1, 2, 3):
        diagonal = diagonal + roll(links[d - 1], -d)

    edges = [[roll(link, -s) for link in links] for s in range(segs)]
    at_lo_wide = jnp.concatenate([at_lo] * 3, axis=1)
    loads[2].wait()
    loads[3].wait()

    table = send_buf[...]
    for copy in copies:
        copy.wait_recv()
    for d in range(1, ncells):
        table = table + recv_buf[d - 1]
    table = [table[k * groups : (k + 1) * groups] for k in range(9)]
    for k in (0, 3, 5):
        table[k] = table[k] + diagonal
    for k in range(3):
        table[6 + k] = table[6 + k] + source[k]
    well_top = [jnp.max(jnp.abs(table[6 + k])) for k in range(3)]

    mats = [[roll(table[k], -s) for k in range(6)] for s in range(segs)]
    vecs = [[roll(table[6 + k], -s) for k in range(3)] for s in range(segs)]
    inverses, partial = [None] * segs, [None] * segs
    for s in range(segs - 1, -1, -1):
        inverses[s] = invert3(mats[s])
        partial[s] = apply3(inverses[s], vecs[s])
        for d in (1, 2, 3):
            if s - d >= 0:
                c = edges[s][d - 1]
                c2 = c * c
                mats[s - d] = [a - c2 * i for a, i in zip(mats[s - d], inverses[s])]
                vecs[s - d] = [r + c * y for r, y in zip(vecs[s - d], partial[s])]
    found = [partial[0]]
    for s in range(1, segs):
        near = [d for d in (3, 2, 1) if s - d >= 0]
        pull = [
            functools.reduce(
                lambda a, b: a + b, [edges[s][d - 1] * found[s - d][k] for d in near]
            )
            for k in range(3)
        ]
        found.append([y + x for y, x in zip(partial[s], apply3(inverses[s], pull))])
    solved = []
    for k in range(3):
        out = found[0][k]
        for s in range(1, segs):
            out = jnp.where(seg == s, roll(found[s][k], s), out)
        solved.append(out)

    mine = iota((groups, targets), 0) == me
    for k in range(3):
        row = jnp.sum(jnp.where(mine, solved[k], F32(0.0)), axis=0, keepdims=True)
        for j in range(owned):
            well_ref[k, j : j + 1, :] = row[:, j * segs : (j + 1) * segs]

    delta = apply3(kmat, table_values(solved))
    corrected, tops = [], []
    for k in range(3):
        spread = jnp.concatenate(
            [jnp.where(at_hi, p, F32(0.0)).astype(BF16) for p in split3(delta[k])], axis=1
        )
        fixed = resid_ref[k] - dot_nt(spread, at_lo_wide)
        corrected.append(fixed)
        tops.append(jnp.max(jnp.abs(fixed)))
    tops = tops + well_top

    lane = iota((1, LANES), 1)
    top = jnp.zeros((1, LANES), F32)
    for k in range(6):
        top = jnp.where(lane == k, tops[k], top)
    top_send[...] = top
    sends = []
    for i, (dc, dw) in enumerate(peers):
        copy = pltpu.make_async_remote_copy(
            src_ref=top_send,
            dst_ref=top_recv.at[i],
            send_sem=top_send_sem,
            recv_sem=top_recv_sem,
            device_id=device(dc, dw),
            device_id_type=MESH,
        )
        copy.start()
    for a in range(3):
        step_ref[a] = sum(inv_ref[3 * a + b] * corrected[b] for b in range(3))
    pltpu.make_async_copy(top_recv, top_recv, top_recv_sem).wait()
    top = jnp.maximum(top, jnp.max(top_recv[...], axis=0))
    top_ref[...] = top
    for copy in copies:
        copy.wait_send()
    pltpu.make_async_copy(top_recv, top_recv, top_send_sem).wait()


def finish(step_in, well_in, top_in, step_ref, well_ref, max_ref):
    top = top_in[...]
    scale = 1.0 / jnp.maximum(F32(1.0), top)
    for k in range(3):
        step_ref[k] = step_in[k] * scale[:, k : k + 1]
    well_ref[...] = well_in[...]
    lane = iota(top.shape, 1)
    for k in range(6):
        max_ref[k] = jnp.max(jnp.where(lane == k, top, F32(0.0)))


def on_device(ncells, nwells, *args):
    (
        cell_state,
        cell_residual,
        cell_block,
        block_inverse,
        perf_cells,
        perf_count,
        perf_index,
        seg_parent,
        seg_cond,
        seg_state,
        seg_source,
    ) = args
    shard = cell_state.shape[2]
    rows = shard // LANES
    wells, slots = perf_cells.shape[1:]
    segs = seg_parent.shape[2]
    owned = wells // ncells
    total = owned * slots
    targets = owned * segs
    others = ncells * nwells - 1

    def planes(x):
        return x.reshape(x.shape[0], rows, LANES)

    vmem = pl.BlockSpec(memory_space=pltpu.VMEM)
    hbm = pl.BlockSpec(memory_space=pltpu.HBM)
    raw, found, top = pl.pallas_call(
        functools.partial(kernel, ncells, nwells),
        out_shape=(
            pltpu.VMEM((3, rows, LANES), F32),
            pltpu.VMEM((3, owned, segs), F32),
            pltpu.VMEM((1, LANES), F32),
        ),
        in_specs=[hbm] * 4 + [vmem] * 7,
        out_specs=(vmem, vmem, vmem),
        scratch_shapes=[
            pltpu.VMEM((3, rows, LANES), F32),
            pltpu.VMEM((9, rows, LANES), F32),
            pltpu.VMEM((3, rows, LANES), F32),
            pltpu.VMEM((9, rows, LANES), F32),
            pltpu.SemaphoreType.DMA((4,)),
            pltpu.VMEM((8, total), F32),
            pltpu.VMEM((7, ncells, targets), F32),
            pltpu.VMEM((ncells, targets), jnp.int32),
            pltpu.VMEM((9 * ncells, targets), F32),
            pltpu.VMEM((ncells - 1, 9 * ncells, targets), F32),
            pltpu.VMEM((1, LANES), F32),
            pltpu.VMEM((others, 1, LANES), F32),
            pltpu.SemaphoreType.DMA((ncells - 1,)),
            pltpu.SemaphoreType.DMA((ncells - 1,)),
            pltpu.SemaphoreType.DMA,
            pltpu.SemaphoreType.DMA,
        ],
        compiler_params=pltpu.CompilerParams(collective_id=0, has_side_effects=True),
    )(
        planes(cell_state),
        planes(cell_block),
        planes(cell_residual),
        planes(block_inverse),
        perf_cells[0],
        perf_count,
        perf_index[0],
        seg_parent[0],
        seg_cond[0],
        seg_state[:, 0],
        seg_source[:, 0],
    )
    step, well, top = pl.pallas_call(
        finish,
        out_shape=(
            jax.ShapeDtypeStruct((3, rows, LANES), F32),
            jax.ShapeDtypeStruct((3, owned, segs), F32),
            jax.ShapeDtypeStruct((6,), F32),
        ),
        in_specs=[vmem] * 3,
        out_specs=(vmem, vmem, pl.BlockSpec(memory_space=pltpu.SMEM)),
    )(*[pltpu.with_memory_space_constraint(x, pltpu.VMEM) for x in (raw, found, top)])
    return (step.reshape(3, 1, shard), well[:, None], top)


def solution(mesh):
    in_specs = (
        P(None, "wells", "cells"),
        P(None, "wells", "cells"),
        P(None, "wells", "cells"),
        P(None, "wells", "cells"),
        P("wells", None, None),
        P("wells", None),
        P("wells", None, None),
        P("wells", None, None),
        P("wells", None, None),
        P(None, "wells", None, None),
        P(None, "wells", None, None),
    )
    out_specs = (P(None, "wells", "cells"), P(None, "wells", "cells", None), P())
    return jax.shard_map(
        functools.partial(on_device, mesh.shape["cells"], mesh.shape["wells"]),
        mesh=mesh,
        in_specs=in_specs,
        out_specs=out_specs,
        check_vma=False,
    )
```

```python
import functools

import jax
import jax.numpy as jnp
from jax import lax
from jax.experimental import pallas as pl
from jax.experimental.pallas import tpu as pltpu
from jax.sharding import PartitionSpec as P

MESH = pl.DeviceIdType.MESH
F32 = jnp.float32
BF16 = jnp.bfloat16
LANES = 128


def iota(shape, axis):
    return lax.broadcasted_iota(jnp.int32, shape, axis)


def split3(x):
    high = x.astype(BF16).astype(F32)
    rest = x - high
    mid = rest.astype(BF16).astype(F32)
    return high, mid, rest - mid


def dot(a, b):
    return lax.dot_general(a, b, (((1,), (0,)), ((), ())), preferred_element_type=F32)


def dot_nt(a, b):
    return lax.dot_general(a, b, (((1,), (1,)), ((), ())), preferred_element_type=F32)


def ones_where(cond):
    return jnp.where(cond, F32(1.0), F32(0.0)).astype(BF16)


def most(x):
    return jnp.max(jnp.max(jnp.abs(x), axis=0, keepdims=True), axis=1, keepdims=True)


def invert3(a):
    a00, a01, a02, a11, a12, a22 = a
    q0 = 1.0 / a00
    l1 = a01 * q0
    l2 = a02 * q0
    b12 = a12 - l1 * a02
    b22 = a22 - l2 * a02
    q1 = a00 * (1.0 / (a00 * a11 - a01 * a01))
    m = b12 * q1
    i22 = 1.0 / (b22 - m * b12)
    i12 = -m * i22
    i11 = q1 - m * i12
    i02 = -(l1 * i12 + l2 * i22)
    i01 = -(l1 * i11 + l2 * i12)
    i00 = q0 - (l1 * i01 + l2 * i02)
    return (i00, i01, i02, i11, i12, i22)


def apply3(a, v):
    a00, a01, a02, a11, a12, a22 = a
    x, y, z = v
    return (
        a00 * x + a01 * y + a02 * z,
        a01 * x + a11 * y + a12 * z,
        a02 * x + a12 * y + a22 * z,
    )


def kernel(
    ncells,
    nwells,
    state_hbm,
    jac_hbm,
    resid_hbm,
    inv_hbm,
    cells_ref,
    count_ref,
    index_ref,
    parent_ref,
    cond_ref,
    segstate_ref,
    source_ref,
    step_ref,
    well_ref,
    top_ref,
    state_ref,
    jac_ref,
    resid_ref,
    inv_ref,
    load_sem,
    feat_scr,
    fold_scr,
    fold_int,
    send_buf,
    recv_buf,
    top_send,
    top_recv,
    send_sem,
    recv_sem,
    top_send_sem,
    top_recv_sem,
):
    loads = [
        pltpu.make_async_copy(src, dst, load_sem.at[i])
        for i, (src, dst) in enumerate(
            (
                (state_hbm, state_ref),
                (jac_hbm, jac_ref),
                (resid_hbm, resid_ref),
                (inv_hbm, inv_ref),
            )
        )
    ]
    for load in loads:
        load.start()
    me = lax.axis_index("cells")
    region = lax.axis_index("wells")
    peers = [
        (dc, dw) for dc in range(ncells) for dw in range(nwells) if (dc, dw) != (0, 0)
    ]

    def device(dc, dw):
        return (lax.rem(me + dc, ncells), lax.rem(region + dw, nwells))

    barrier = pltpu.get_barrier_semaphore()
    greeted = [(dc, dw) for dc, dw in peers if dc == 0 or dw == 0]
    for dc, dw in greeted:
        pl.semaphore_signal(barrier, inc=1, device_id=device(dc, dw), device_id_type=MESH)

    wells, slots = cells_ref.shape
    segs = parent_ref.shape[1]
    rows = state_ref.shape[1]
    shard = rows * LANES
    groups = ncells
    owned = wells // groups
    per = owned * slots // ncells
    total = groups * per
    targets = owned * segs

    offset = cells_ref[...] - me * shard
    inside = (offset >= 0) & (offset < shard)
    mask = ones_where(inside)
    before = ones_where(iota((slots, slots), 0) < iota((slots, slots), 1))
    wi, wj = iota((wells, wells), 0), iota((wells, wells), 1)
    above = ones_where((wi // owned == wj // owned) & (wj < wi))
    full = jnp.ones((slots, slots), BF16)
    rank = dot(mask, before) + dot(dot(above, mask).astype(BF16), full)
    rank = jnp.where(inside, rank, F32(-1.0))
    counts = dot(
        jnp.where(wi == wj, count_ref[...].astype(F32), F32(0.0)).astype(BF16),
        jnp.ones((wells, slots), BF16),
    )
    live = iota((wells, slots), 1).astype(F32) < counts
    weight = jnp.where(live, index_ref[...], F32(0.0))
    hi = jnp.where(inside, offset // LANES, 0).astype(F32)
    lo = jnp.where(inside, offset % LANES, 0).astype(F32)
    slot_seg = iota((1, slots), 1) // (slots // segs)
    parts = (hi, lo) + split3(weight)
    sub = iota((8, slots), 0)
    order = iota((per, slots), 0).astype(F32)
    for g in range(groups):
        feats, picks = [], []
        for j in range(owned):
            w = g * owned + j
            f = jnp.broadcast_to((slot_seg + j * segs).astype(F32), (8, slots))
            for k, part in enumerate(parts):
                f = jnp.where(sub == k, part[w : w + 1], f)
            feats.append(f)
            picks.append(ones_where(rank[w : w + 1] == order))
        feat_scr[:, g * per : (g + 1) * per] = dot_nt(
            jnp.concatenate(feats, axis=1).astype(BF16), jnp.concatenate(picks, axis=1)
        )

    slot_hi = feat_scr[0:1]
    slot_lo = feat_scr[1:2]
    slot_weight = feat_scr[2:3] + feat_scr[3:4] + feat_scr[4:5]
    slot_target = feat_scr[5:6]
    at_lo = ones_where(iota((LANES, total), 0).astype(F32) == slot_lo)
    at_hi = iota((rows, total), 0).astype(F32) == slot_hi
    at_target = ones_where(iota((targets, total), 0).astype(F32) == slot_target)
    in_group = iota((groups, total), 1) // per == iota((groups, total), 0)
    at_lo3 = jnp.concatenate([at_lo] * 3, axis=0)

    def cell_values(values):
        pieces = jnp.concatenate([p.astype(BF16) for p in split3(values)], axis=1)
        spread = dot(pieces, at_lo3)
        return jnp.sum(jnp.where(at_hi, spread, F32(0.0)), axis=0, keepdims=True)

    def table_values(tables):
        pieces = [split3(t) for t in tables]
        stacked = jnp.concatenate([p[i] for i in range(3) for p in pieces], axis=0)
        spread = dot(stacked.astype(BF16), at_target)
        size = len(tables) * groups
        spread = spread[:size] + spread[size : 2 * size] + spread[2 * size :]
        return [
            jnp.sum(
                jnp.where(in_group, spread[k * groups : (k + 1) * groups], F32(0.0)),
                axis=0,
                keepdims=True,
            )
            for k in range(len(tables))
        ]

    def fold(read, scratch):
        for j in range(owned):
            scratch[:, j * segs : (j + 1) * segs] = read(pl.ds(j, groups, stride=owned))
        return scratch[...]

    seg_state = [
        fold(lambda s, k=k: segstate_ref[k, s, :], fold_scr.at[k]) for k in range(3)
    ]
    source = [fold(lambda s, k=k: source_ref[k, s, :], fold_scr.at[3 + k]) for k in range(3)]
    cond = fold(lambda s: cond_ref[s, :], fold_scr.at[6])
    parent = fold(lambda s: parent_ref[s, :], fold_int)

    loads[0].wait()
    loads[1].wait()
    state_at = [cell_values(state_ref[k]) for k in range(3)]
    jac = [cell_values(jac_ref[k]) for k in range(9)]
    differ = [a - b for a, b in zip(state_at, table_values(seg_state))]
    kmat = []
    for a in range(3):
        for b in range(a, 3):
            entry = sum(jac[3 * a + c] * jac[3 * b + c] for c in range(3))
            kmat.append((entry + 1.0 if a == b else entry) * slot_weight)
    flow = apply3(kmat, differ)
    values = [split3(v) for v in kmat + list(flow)]
    placed = jnp.concatenate(
        [jnp.where(in_group, v[i], F32(0.0)) for i in range(3) for v in values], axis=0
    )
    summed = dot_nt(placed.astype(BF16), at_target)
    size = 9 * groups
    send_buf[...] = summed[:size] + summed[size : 2 * size] + summed[2 * size :]

    pl.semaphore_wait(barrier, len(greeted))
    copies = []
    for d in range(1, ncells):
        copy = pltpu.make_async_remote_copy(
            src_ref=send_buf,
            dst_ref=recv_buf.at[d - 1],
            send_sem=send_sem.at[d - 1],
            recv_sem=recv_sem.at[d - 1],
            device_id=device(d, 0),
            device_id_type=MESH,
        )
        copy.start()
        copies.append(copy)

    seg = iota((groups, targets), 1) % segs
    dist = seg - parent
    links = [jnp.where((dist == d) & (seg >= 1), cond, F32(0.0)) for d in (1, 2, 3)]

    def roll(x, shift):
        shift = shift % targets
        return pltpu.roll(x, shift, 1) if shift else x

    diagonal = 1.0 + links[0] + links[1] + links[2]
    for d in (1, 2, 3):
        diagonal = diagonal + roll(links[d - 1], -d)

    edges = [[roll(link, -s) for link in links] for s in range(segs)]
    at_lo_wide = jnp.concatenate([at_lo] * 3, axis=1)
    loads[2].wait()
    loads[3].wait()

    table = send_buf[...]
    for copy in copies:
        copy.wait_recv()
    for d in range(1, ncells):
        table = table + recv_buf[d - 1]
    table = [table[k * groups : (k + 1) * groups] for k in range(9)]
    for k in (0, 3, 5):
        table[k] = table[k] + diagonal
    for k in range(3):
        table[6 + k] = table[6 + k] + source[k]
    well_top = [most(table[6 + k]) for k in range(3)]

    mats = [[roll(table[k], -s) for k in range(6)] for s in range(segs)]
    vecs = [[roll(table[6 + k], -s) for k in range(3)] for s in range(segs)]
    inverses, partial = [None] * segs, [None] * segs
    for s in range(segs - 1, -1, -1):
        inverses[s] = invert3(mats[s])
        partial[s] = apply3(inverses[s], vecs[s])
        for d in (1, 2, 3):
            if s - d >= 0:
                c = edges[s][d - 1]
                c2 = c * c
                mats[s - d] = [a - c2 * i for a, i in zip(mats[s - d], inverses[s])]
                vecs[s - d] = [r + c * y for r, y in zip(vecs[s - d], partial[s])]
    found = [partial[0]]
    for s in range(1, segs):
        near = [d for d in (3, 2, 1) if s - d >= 0]
        pull = [
            functools.reduce(
                lambda a, b: a + b, [edges[s][d - 1] * found[s - d][k] for d in near]
            )
            for k in range(3)
        ]
        found.append([y + x for y, x in zip(partial[s], apply3(inverses[s], pull))])
    solved = []
    for k in range(3):
        out = found[0][k]
        for s in range(1, segs):
            out = jnp.where(seg == s, roll(found[s][k], s), out)
        solved.append(out)

    mine = iota((groups, targets), 0) == me
    for k in range(3):
        row = jnp.sum(jnp.where(mine, solved[k], F32(0.0)), axis=0, keepdims=True)
        for j in range(owned):
            well_ref[k, j : j + 1, :] = row[:, j * segs : (j + 1) * segs]

    delta = apply3(kmat, table_values(solved))
    corrected, tops = [], []
    for k in range(3):
        spread = jnp.concatenate(
            [jnp.where(at_hi, p, F32(0.0)).astype(BF16) for p in split3(delta[k])], axis=1
        )
        fixed = resid_ref[k] - dot_nt(spread, at_lo_wide)
        corrected.append(fixed)
        tops.append(most(fixed))
    tops = tops + well_top

    lane = iota((1, LANES), 1)
    top = jnp.zeros((1, LANES), F32)
    for k in range(6):
        top = jnp.where(lane == k, tops[k], top)
    top_send[...] = top
    sends = []
    for i, (dc, dw) in enumerate(peers):
        copy = pltpu.make_async_remote_copy(
            src_ref=top_send,
            dst_ref=top_recv.at[i],
            send_sem=top_send_sem,
            recv_sem=top_recv_sem,
            device_id=device(dc, dw),
            device_id_type=MESH,
        )
        copy.start()
    for a in range(3):
        step_ref[a] = sum(inv_ref[3 * a + b] * corrected[b] for b in range(3))
    pltpu.make_async_copy(top_recv, top_recv, top_recv_sem).wait()
    top = jnp.maximum(top, jnp.max(top_recv[...], axis=0))
    top_ref[...] = top
    for copy in copies:
        copy.wait_send()
    pltpu.make_async_copy(top_recv, top_recv, top_send_sem).wait()


def finish(step_in, well_in, top_in, step_ref, well_ref, max_ref):
    top = top_in[...]
    scale = 1.0 / jnp.maximum(F32(1.0), top)
    for k in range(3):
        step_ref[k] = step_in[k] * scale[:, k : k + 1]
    well_ref[...] = well_in[...]
    lane = iota(top.shape, 1)
    for k in range(6):
        max_ref[k] = jnp.max(jnp.where(lane == k, top, F32(0.0)))


def on_device(ncells, nwells, *args):
    (
        cell_state,
        cell_residual,
        cell_block,
        block_inverse,
        perf_cells,
        perf_count,
        perf_index,
        seg_parent,
        seg_cond,
        seg_state,
        seg_source,
    ) = args
    shard = cell_state.shape[2]
    rows = shard // LANES
    wells, slots = perf_cells.shape[1:]
    segs = seg_parent.shape[2]
    owned = wells // ncells
    total = owned * slots
    targets = owned * segs
    others = ncells * nwells - 1

    def planes(x):
        return x.reshape(x.shape[0], rows, LANES)

    vmem = pl.BlockSpec(memory_space=pltpu.VMEM)
    hbm = pl.BlockSpec(memory_space=pltpu.HBM)
    raw, found, top = pl.pallas_call(
        functools.partial(kernel, ncells, nwells),
        out_shape=(
            pltpu.VMEM((3, rows, LANES), F32),
            pltpu.VMEM((3, owned, segs), F32),
            pltpu.VMEM((1, LANES), F32),
        ),
        in_specs=[hbm] * 4 + [vmem] * 7,
        out_specs=(vmem, vmem, vmem),
        scratch_shapes=[
            pltpu.VMEM((3, rows, LANES), F32),
            pltpu.VMEM((9, rows, LANES), F32),
            pltpu.VMEM((3, rows, LANES), F32),
            pltpu.VMEM((9, rows, LANES), F32),
            pltpu.SemaphoreType.DMA((4,)),
            pltpu.VMEM((8, total), F32),
            pltpu.VMEM((7, ncells, targets), F32),
            pltpu.VMEM((ncells, targets), jnp.int32),
            pltpu.VMEM((9 * ncells, targets), F32),
            pltpu.VMEM((ncells - 1, 9 * ncells, targets), F32),
            pltpu.VMEM((1, LANES), F32),
            pltpu.VMEM((others, 1, LANES), F32),
            pltpu.SemaphoreType.DMA((ncells - 1,)),
            pltpu.SemaphoreType.DMA((ncells - 1,)),
            pltpu.SemaphoreType.DMA,
            pltpu.SemaphoreType.DMA,
        ],
        compiler_params=pltpu.CompilerParams(collective_id=0, has_side_effects=True),
    )(
        planes(cell_state),
        planes(cell_block),
        planes(cell_residual),
        planes(block_inverse),
        perf_cells[0],
        perf_count,
        perf_index[0],
        seg_parent[0],
        seg_cond[0],
        seg_state[:, 0],
        seg_source[:, 0],
    )
    step, well, top = pl.pallas_call(
        finish,
        out_shape=(
            jax.ShapeDtypeStruct((3, rows, LANES), F32),
            jax.ShapeDtypeStruct((3, owned, segs), F32),
            jax.ShapeDtypeStruct((6,), F32),
        ),
        in_specs=[vmem] * 3,
        out_specs=(vmem, vmem, pl.BlockSpec(memory_space=pltpu.SMEM)),
    )(*[pltpu.with_memory_space_constraint(x, pltpu.VMEM) for x in (raw, found, top)])
    return (step.reshape(3, 1, shard), well[:, None], top)


def solution(mesh):
    in_specs = (
        P(None, "wells", "cells"),
        P(None, "wells", "cells"),
        P(None, "wells", "cells"),
        P(None, "wells", "cells"),
        P("wells", None, None),
        P("wells", None),
        P("wells", None, None),
        P("wells", None, None),
        P("wells", None, None),
        P(None, "wells", None, None),
        P(None, "wells", None, None),
    )
    out_specs = (P(None, "wells", "cells"), P(None, "wells", "cells", None), P())
    return jax.shard_map(
        functools.partial(on_device, mesh.shape["cells"], mesh.shape["wells"]),
        mesh=mesh,
        in_specs=in_specs,
        out_specs=out_specs,
        check_vma=False,
    )
```
